32 devices in a mesh: cat: 2 (over x), lat: 4 (over y, core), lon: 4 (over z).
Axes of the slice: x: 2, y: 2, z: 4, core: 2. Of those that a mesh axis runs over, the one named last changes fastest.
Arguments:
- thickness: bfloat16 [40, 1024, 2560], P('cat', 'lat', 'lon'), may hold values from 0.099609375 to 4
- area: bfloat16 [40, 1024, 2560], P('cat', 'lat', 'lon'), may hold values from 0.0049743652 to 0.049804688
- ridge_weight: float32 [40], P('cat'), may hold values from 0.2 to 2
- cat_top: int32 [1024, 2560], P('lat', 'lon'), may hold values from 1 to 40
- land_mask: int32 [1024, 2560], P('lat', 'lon'), may hold values 0 or 1
- velocity_u: float32 [1024, 2560], P('lat', 'lon'), may hold values from -1.8 to 1.8
- velocity_v: float32 [1024, 2560], P('lat', 'lon'), may hold values from -1.8 to 1.8
- stress_div: float32 [1024, 2560], P('lat', 'lon'), may hold values from -3 to 3
- stress_ten: float32 [1024, 2560], P('lat', 'lon'), may hold values from -3 to 3
- stress_shear: float32 [1024, 2560], P('lat', 'lon'), may hold values from -3 to 3
- wind_x: float32 [1024, 2560], P('lat', 'lon'), may hold values from -6 to 6
- wind_y: float32 [1024, 2560], P('lat', 'lon'), may hold values from -6 to 6
- water_drag: float32 [1024, 2560], P('lat', 'lon'), may hold values from 0.2 to 2
Outputs:
- new_u: float32 [1024, 2560], P('lat', 'lon')
- new_v: float32 [1024, 2560], P('lat', 'lon')
- new_div: float32 [1024, 2560], P('lat', 'lon')
- new_ten: float32 [1024, 2560], P('lat', 'lon')
- new_shear: float32 [1024, 2560], P('lat', 'lon')
The draws below stay inside these ranges and needn't reach their ends.
Inputs may be any that keep to these rules, and one draw needn't show every extreme that they name: Categories with index cat_top or above are absent from a cell.
All inputs are finite; a program needn't handle non-finite values. No bound on the sum of `land_mask` on one device may be relied on, other than what follows from the above.
Results may differ from the reference program's by a relative error of at most 0.0003.
Values sent between devices are 32-bit elements; how exact they have to be, the bound alone decides.
No kernel may reach another device: no remote copies, remote signals or barrier semaphores. Data moves between devices by JAX's collectives and lax.ppermute only.
A program may use at most 128 MiB of HBM per device.

```python
import math
import jax
import jax.numpy as jnp
from jax import lax

NCAT = 40
SUB = 4
NLAT = 1024
NLON = 2560


def with_ends(entries, stream_key, least, high):
    shape = entries.shape
    spot = [jax.random.randint(jax.random.fold_in(stream_key, axis), (), 0, shape[axis]) for axis in range(len(shape))]
    entries = entries.at[tuple(spot)].set(least)
    longest = shape.index(max(shape))
    spot[longest] = (spot[longest] + 1) % shape[longest]
    return entries.at[tuple(spot)].set(high)


def shard_levels(rng, extent, cuts, low, high):
    factor_of = 1.0
    for axis_at, shards_of in cuts:
        steps = jax.random.uniform(jax.random.fold_in(jax.random.fold_in(rng, 6), axis_at), (shards_of,), jnp.float32, low / len(cuts), high / len(cuts))
        factor_of = factor_of * jnp.repeat(jnp.exp(steps), extent[axis_at] // shards_of).reshape((-1,) + (1,) * (len(extent) - 1 - axis_at))
    return factor_of


def noise(own_key, shape, deviation, limit, cuts=(), dtype=jnp.bfloat16):
    drawn = jax.random.normal(own_key, shape, jnp.float32) * deviation
    if len(cuts) > 0:
        drawn = shard_levels(own_key, shape, cuts, -0.22, 0.18) * drawn
    return jnp.clip(drawn, min=-limit, max=limit).astype(dtype)


def setup_inputs(seed: int = 0) -> dict:
    streams_of = jax.random.split(jax.random.key(seed), 14)
    return {
        "thickness": jnp.clip(jnp.exp(math.log(4.0) - 3.6927934 * jax.random.uniform(streams_of[0], (NCAT, NLAT, NLON), jnp.float32) ** shard_levels(streams_of[0], (NCAT, NLAT, NLON), ((0, 2), (1, 4), (2, 4)), -0.2, 0.2)), 0.099609375, 4.0).astype(jnp.bfloat16),
        "area": jnp.clip(jnp.exp(math.log(0.049804688) - 2.3038113 * jax.random.uniform(streams_of[1], (NCAT, NLAT, NLON), jnp.float32) ** shard_levels(streams_of[1], (NCAT, NLAT, NLON), ((0, 2), (1, 4), (2, 4)), -0.2, 0.2)), 0.0049743652, 0.049804688).astype(jnp.bfloat16),
        "ridge_weight": jnp.clip(jnp.exp(math.log(2.0) - 2.3025851 * jax.random.uniform(streams_of[2], (NCAT,), jnp.float32) ** shard_levels(streams_of[2], (NCAT,), ((0, 2),), -0.2, 0.2)), 0.2, 2.0),
        "cat_top": with_ends(jax.random.randint(streams_of[3], (NLAT, NLON), 1, NCAT + 1), jax.random.fold_in(streams_of[3], 1), 1, NCAT).astype(jnp.int32),
        "land_mask": with_ends((jax.random.randint(streams_of[4], (NLAT, NLON), 0, 10) < 9).astype(jnp.int32), jax.random.fold_in(streams_of[4], 1), 0, 1),
        "velocity_u": noise(streams_of[5], (NLAT, NLON), 0.3, 1.8, ((0, 4), (1, 4)), jnp.float32),
        "velocity_v": noise(streams_of[6], (NLAT, NLON), 0.3, 1.8, ((0, 4), (1, 4)), jnp.float32),
        "stress_div": noise(streams_of[7], (NLAT, NLON), 0.5, 3.0, ((0, 4), (1, 4)), jnp.float32),
        "stress_ten": noise(streams_of[8], (NLAT, NLON), 0.5, 3.0, ((0, 4), (1, 4)), jnp.float32),
        "stress_shear": noise(streams_of[9], (NLAT, NLON), 0.5, 3.0, ((0, 4), (1, 4)), jnp.float32),
        "wind_x": noise(streams_of[10], (NLAT, NLON), 1.0, 6.0, ((0, 4), (1, 4)), jnp.float32),
        "wind_y": noise(streams_of[11], (NLAT, NLON), 1.0, 6.0, ((0, 4), (1, 4)), jnp.float32),
        "water_drag": jnp.clip(jnp.exp(math.log(2.0) - 2.3025851 * jax.random.uniform(streams_of[12], (NLAT, NLON), jnp.float32) ** shard_levels(streams_of[12], (NLAT, NLON), ((0, 4), (1, 4)), -0.2, 0.2)), 0.2, 2.0),
    }


ELASTIC = 2.0
ECC_SQUARED = 4.0
DELTA_FLOOR = 0.05
CORIOLIS = 0.5

def slopes(along, across):
    return (0.5 * (along[:, :, 2:] - along[:, :, :-2]), 0.5 * (across[:, 2:, :] - across[:, :-2, :]))

def global_pad(along_stack, across_stack):
    along = jnp.pad(along_stack, ((0, 0), (0, 0), (1, 1)), mode='wrap')
    across = jnp.pad(across_stack, ((0, 0), (1, 1), (0, 0)))
    return (along, across)

def subcycle(velocity, stresses, statics):
    strength, mass, concentration, drag, push_x, push_y, wet = statics
    along, across = global_pad(velocity, velocity)
    ddx, ddy = slopes(along, across)
    divergence = ddx[0] + ddy[1]
    tension = ddx[0] - ddy[1]
    shearing = ddy[0] + ddx[1]
    delta = jnp.sqrt(divergence * divergence + (tension * tension + shearing * shearing) / ECC_SQUARED + DELTA_FLOOR * DELTA_FLOOR)
    relax = 1.0 / (1.0 + ELASTIC)
    viscous = ELASTIC * strength / delta
    first = wet * (stresses[0] + viscous * (divergence - delta)) * relax
    second = wet * (stresses[1] + viscous * tension / ECC_SQUARED) * relax
    cross = wet * (stresses[2] + viscous * shearing / ECC_SQUARED) * relax
    normal_x = 0.5 * (first + second)
    normal_y = 0.5 * (first - second)
    along_s, across_s = global_pad(jnp.stack([normal_x, cross]), jnp.stack([cross, normal_y]))
    sdx, sdy = slopes(along_s, across_s)
    force_x = sdx[0] + sdy[0]
    force_y = sdx[1] + sdy[1]
    denom = mass + drag + 1.0 - wet
    speed_u = wet * (mass * velocity[0] + force_x + concentration * push_x + CORIOLIS * mass * velocity[1]) / denom
    speed_v = wet * (mass * velocity[1] + force_y + concentration * push_y - CORIOLIS * mass * velocity[0]) / denom
    return (jnp.stack([speed_u, speed_v]), jnp.stack([first, second, cross]))

def reference(thickness, area, ridge_weight, cat_top, land_mask, velocity_u, velocity_v, stress_div, stress_ten, stress_shear, wind_x, wind_y, water_drag):

    def accumulate(level, carry):
        strength, mass, concentration = carry
        height = lax.dynamic_index_in_dim(thickness, level, 0, keepdims=False).astype(jnp.float32)
        present = (level < cat_top).astype(jnp.float32)
        cover = lax.dynamic_index_in_dim(area, level, 0, keepdims=False).astype(jnp.float32) * present
        weight = lax.dynamic_index_in_dim(ridge_weight, level, 0, keepdims=False)
        return (strength + weight * cover * height * height, mass + cover * height, concentration + cover)
    zeros = jnp.zeros(cat_top.shape, jnp.float32)
    strength, mass, concentration = lax.fori_loop(jnp.int32(0), jnp.int32(NCAT), accumulate, (zeros, zeros, zeros))
    wet = land_mask.astype(jnp.float32)
    statics = (strength, mass, concentration, water_drag, wind_x, wind_y, wet)
    velocity = jnp.stack([velocity_u, velocity_v])
    stresses = jnp.stack([stress_div, stress_ten, stress_shear])
    for step in range(SUB):
        velocity, stresses = subcycle(velocity, stresses, statics)
    return (velocity[0], velocity[1], stresses[0], stresses[1], stresses[2])
```

```python
import jax
import jax.numpy as jnp
from jax import lax
from jax.sharding import PartitionSpec as P

SUB = 4


ELASTIC = 2.0
ECC_SQUARED = 4.0
DELTA_FLOOR = 0.05
CORIOLIS = 0.5


def extended(cells, sides, width, closed):
    for axis, dim in sides:
        count = lax.axis_size(axis)
        ends = count if closed else count - 1
        head = lax.slice_in_dim(cells, 0, width, axis=dim)
        tail = lax.slice_in_dim(cells, cells.shape[dim] - width, cells.shape[dim], axis=dim)
        cells = jnp.concatenate(
            [
                lax.ppermute(tail, axis, [(i, (i + 1) % count) for i in range(ends)]),
                cells,
                lax.ppermute(head, axis, [((i + 1) % count, i) for i in range(ends)]),
            ],
            axis=dim,
        )
    return cells


def slopes(along, across):
    return (
        0.5 * (along[:, :, 2:] - along[:, :, :-2]),
        0.5 * (across[:, 2:, :] - across[:, :-2, :]),
    )


def local_pad(along_stack, across_stack):
    along = jnp.pad(along_stack, ((0, 0), (0, 0), (1, 1)))
    across = jnp.pad(across_stack, ((0, 0), (1, 1), (0, 0)))
    return (along, across)


def subcycle(velocity, stresses, statics, velocity_pad, stress_pad):
    strength, mass, concentration, drag, push_x, push_y, wet = statics
    along, across = velocity_pad(velocity, velocity)
    ddx, ddy = slopes(along, across)
    divergence = ddx[0] + ddy[1]
    tension = ddx[0] - ddy[1]
    shearing = ddy[0] + ddx[1]
    delta = jnp.sqrt(
        divergence * divergence
        + (tension * tension + shearing * shearing) / ECC_SQUARED
        + DELTA_FLOOR * DELTA_FLOOR
    )
    relax = 1.0 / (1.0 + ELASTIC)
    viscous = ELASTIC * strength / delta
    first = wet * (stresses[0] + viscous * (divergence - delta)) * relax
    second = wet * (stresses[1] + viscous * tension / ECC_SQUARED) * relax
    cross = wet * (stresses[2] + viscous * shearing / ECC_SQUARED) * relax
    normal_x = 0.5 * (first + second)
    normal_y = 0.5 * (first - second)
    along_s, across_s = stress_pad(jnp.stack([normal_x, cross]), jnp.stack([cross, normal_y]))
    sdx, sdy = slopes(along_s, across_s)
    force_x = sdx[0] + sdy[0]
    force_y = sdx[1] + sdy[1]
    denom = mass + drag + 1.0 - wet
    speed_u = (
        wet
        * (mass * velocity[0] + force_x + concentration * push_x + CORIOLIS * mass * velocity[1])
        / denom
    )
    speed_v = (
        wet
        * (mass * velocity[1] + force_y + concentration * push_y - CORIOLIS * mass * velocity[0])
        / denom
    )
    return (jnp.stack([speed_u, speed_v]), jnp.stack([first, second, cross]))


def shards(
    thickness,
    area,
    ridge_weight,
    cat_top,
    land_mask,
    velocity_u,
    velocity_v,
    stress_div,
    stress_ten,
    stress_shear,
    wind_x,
    wind_y,
    water_drag,
):
    local_cats = thickness.shape[0]
    level = lax.axis_index("cat") * local_cats + lax.broadcasted_iota(jnp.int32, thickness.shape, 0)
    present = (level < cat_top[None]).astype(jnp.float32)
    height = thickness.astype(jnp.float32)
    cover = area.astype(jnp.float32) * present
    weighted = ridge_weight[:, None, None] * cover * height * height
    partial = jnp.stack(
        [jnp.sum(weighted, axis=0), jnp.sum(cover * height, axis=0), jnp.sum(cover, axis=0)]
    )
    count = lax.axis_size("cat")
    totals = partial
    for shift in range(1, count):
        totals = totals + lax.ppermute(
            partial, "cat", [(i, (i + shift) % count) for i in range(count)]
        )
    strength, mass, concentration = totals
    wet = land_mask.astype(jnp.float32)
    margin = 2 * SUB
    bundle = jnp.stack(
        [
            strength,
            mass,
            concentration,
            water_drag,
            wind_x,
            wind_y,
            wet,
            velocity_u,
            velocity_v,
            stress_div,
            stress_ten,
            stress_shear,
        ]
    )
    widened = extended(bundle, (("lon", 2),), margin, True)
    padded = extended(widened, (("lat", 1),), margin, False)
    statics = tuple((padded[index] for index in range(7)))
    velocity = padded[7:9]
    stresses = padded[9:12]
    for step in range(SUB):
        velocity, stresses = subcycle(velocity, stresses, statics, local_pad, local_pad)
    rows = velocity.shape[1] - margin
    cols = velocity.shape[2] - margin
    velocity = velocity[:, margin:rows, margin:cols]
    stresses = stresses[:, margin:rows, margin:cols]
    return (velocity[0], velocity[1], stresses[0], stresses[1], stresses[2])


def solution(mesh):
    return jax.shard_map(
        shards,
        mesh=mesh,
        in_specs=(
            P("cat", "lat", "lon"),
            P("cat", "lat", "lon"),
            P("cat"),
            P("lat", "lon"),
            P("lat", "lon"),
            P("lat", "lon"),
            P("lat", "lon"),
            P("lat", "lon"),
            P("lat", "lon"),
            P("lat", "lon"),
            P("lat", "lon"),
            P("lat", "lon"),
            P("lat", "lon"),
        ),
        out_specs=(
            P("lat", "lon"),
            P("lat", "lon"),
            P("lat", "lon"),
            P("lat", "lon"),
            P("lat", "lon"),
        ),
        check_vma=False,
    )
```
